16 devices in a mesh: rep: 4 (over y, z, core), dp: 4 (over x).
Axes of the slice: x: 4, y: 2, z: 1, core: 2. Of those that a mesh axis runs over, the one named last changes fastest.
The devices are a block of a 4x4x8 slice.
Arguments:
- a: bfloat16 [16, 4, 8192, 512], P(('rep', 'dp')), parts along dimension 0
- g: bfloat16 [16, 4, 8192, 1408], P(('rep', 'dp')), parts along dimension 0
Outputs:
- output: bfloat16 [16, 512, 1408], P('rep'), parts along dimension 0
There are 4 independent parts. The reference program is written for one: setup_inputs(seed, part) draws one part's arguments, and reference() takes and returns one part's arrays. A program takes and returns all parts, laid end to end along the dimension named above; each array names one.
All inputs are finite; a program needn't handle non-finite values.
Results may differ from the reference program's by a relative error of at most 0.012.
Values are sent between devices in bfloat16 or wider.
A program may use at most 768 MiB of HBM per device.

```python
import jax
import jax.numpy as jnp
from jax import lax

DEVICES = 4
MATRICES = 4
TOKENS = 8192
D = 512
FF = 1408


def setup_inputs(seed: int = 0, part: int = 0) -> dict:
    ka, kg, ks = (jax.random.fold_in(k, part) for k in jax.random.split(jax.random.key(seed), 3))
    size = 2.0 ** jax.random.uniform(ks, (DEVICES, MATRICES, 1, 1), jnp.float32, -1.0, 1.0)
    a = jax.random.normal(ka, (DEVICES, MATRICES, TOKENS, D), jnp.float32)
    g = size * jax.random.normal(kg, (DEVICES, MATRICES, TOKENS, FF), jnp.float32) * (DEVICES * TOKENS) ** -0.5
    return {"a": a.astype(jnp.bfloat16), "g": g.astype(jnp.bfloat16)}


def reference(a, g):
    def take(so_far, one):
        return so_far + jnp.einsum("ntd,ntf->ndf", *one, preferred_element_type=jnp.float32), None

    return lax.scan(take, jnp.zeros((MATRICES, D, FF), jnp.float32), (a, g))[0].astype(jnp.bfloat16)
```

```python
import functools

import jax
import jax.numpy as jnp
from jax import lax
from jax.experimental import pallas as pl
from jax.experimental.pallas import tpu as pltpu

WIDE = 256
SLOTS = 4
PIECES = 4
RIGHT, LEFT = 0, 1


def kernel(axis, group, a_hbm, g_hbm, out, a_buf, g_buf, first, landed, a_sem, a0_sem, g_sem, g0_sem, send_sem, recv_sem):
    tokens, rows = a_hbm.shape[1:]
    columns = g_hbm.shape[2]
    half = rows // 2
    narrow = columns % WIDE or WIDE
    chunks = 1 + (columns - narrow) // WIDE
    me = lax.axis_index(axis)
    ring = [lax.rem(me + k, group) for k in range(group)]
    peer = (ring[1], ring[group - 1])

    def width(j):
        return narrow if isinstance(j, int) and j == 0 else WIDE

    def start_column(j):
        if isinstance(j, int):
            return 0 if j == 0 else narrow + (j - 1) * WIDE
        return pl.multiple_of(narrow + (j - 1) * WIDE, 128)

    def cols(j):
        return pl.ds(start_column(j), width(j))

    def half_rows(side):
        return pl.ds(side * half, half)

    def matrix(phase, side):
        return ring[(group - 1 - phase) % group] if side == RIGHT else ring[(phase + 1) % group]

    def g_load(m, j, slot):
        step = tokens // PIECES
        for p in range(PIECES):
            rows_p = pl.ds(p * step, step)
            pltpu.make_async_copy(
                g_hbm.at[m, rows_p, cols(j)], g_buf.at[slot, rows_p, pl.ds(0, width(j))], g_sem.at[slot]
            ).start()

    def g_wait(j, slot):
        pltpu.make_async_copy(
            g_hbm.at[0, :, cols(j)], g_buf.at[slot, :, pl.ds(0, width(j))], g_sem.at[slot]
        ).wait()

    def a_load(phase, side):
        pltpu.make_async_copy(
            a_hbm.at[matrix(phase, side), :, half_rows(side)],
            a_buf.at[phase % 2, :, half_rows(side)],
            a_sem.at[phase % 2, side],
        ).start()

    def a_wait(phase, side):
        pltpu.make_async_copy(
            a_hbm.at[0, :, half_rows(side)], a_buf.at[phase % 2, :, half_rows(side)], a_sem.at[phase % 2, side]
        ).wait()

    def piece_copies(side, p):
        step = tokens // PIECES
        rows_p = pl.ds(p * step, step)
        m = matrix(0, side)
        return (
            pltpu.make_async_copy(
                a_hbm.at[m, rows_p, half_rows(side)], a_buf.at[0, rows_p, half_rows(side)], a0_sem.at[side, p]
            ),
            pltpu.make_async_copy(
                g_hbm.at[m, rows_p, cols(0)], g_buf.at[side, rows_p, pl.ds(0, narrow)], g0_sem.at[side, p]
            ),
        )

    def hop(side, n, j):
        if n < group - 1:
            src = (first if n == 0 else landed.at[n - 1]).at[side, j, :, pl.ds(0, width(j))]
            dst = landed.at[n, side, j, :, pl.ds(0, width(j))]
        else:
            k = n - (group - 1)
            m = ring[(group - k) % group] if side == RIGHT else ring[k]
            src = dst = out.at[m, half_rows(side), cols(j)]
        return pltpu.make_async_remote_copy(
            src_ref=src,
            dst_ref=dst,
            send_sem=send_sem.at[side, n, j],
            recv_sem=recv_sem.at[side, n, j],
            device_id={axis: peer[side]},
            device_id_type=pl.DeviceIdType.MESH,
        )

    def arrived(side, n, j):
        if n < group - 1:
            return hop(side, n, j)
        k = n - (group - 1) + 1
        m = ring[(group - k) % group] if side == RIGHT else ring[k % group]
        ref = out.at[m, half_rows(side), cols(j)]
        return pltpu.make_async_remote_copy(
            src_ref=ref,
            dst_ref=ref,
            send_sem=send_sem.at[side, n, j],
            recv_sem=recv_sem.at[side, n, j],
            device_id={axis: peer[side]},
            device_id_type=pl.DeviceIdType.MESH,
        )

    def product(a, g):
        return lax.dot_general(a, g, (((0,), (0,)), ((), ())), preferred_element_type=jnp.float32)

    def pass_on(phase, side, j, term):
        w = width(j)
        if phase == 0:
            first[side, j, :, pl.ds(0, w)] = term.astype(first.dtype)
        else:
            arrived(side, phase - 1, j).wait_recv()
            total = (landed[phase - 1, side, j, :, pl.ds(0, w)].astype(jnp.float32) + term).astype(first.dtype)
            if phase < group - 1:
                landed[phase - 1, side, j, :, pl.ds(0, w)] = total
            else:
                out[me, half_rows(side), cols(j)] = total
        hop(side, phase, j).start()

    split = [True, False, True, False]
    base = [0, 2 * chunks, 3 * chunks, 5 * chunks]
    total_blocks = 6 * chunks

    def slot_of(phase, j, side):
        return (base[phase] + (2 * j + side if split[phase] else j)) % SLOTS

    def refill(phase, j, side):
        def fetch(q, jj, ss):
            g_load(matrix(q, ss), jj, slot_of(q, jj, ss))

        def later(q, flat):
            if split[q]:
                raise AssertionError
            fetch(q, flat, RIGHT)

        if split[phase]:
            if isinstance(j, int):
                flat = 2 * j + side + SLOTS
                if flat < 2 * chunks:
                    fetch(phase, flat // 2, flat % 2)
                else:
                    fetch(phase + 1, flat - 2 * chunks, RIGHT)
                return
            near = chunks - SLOTS // 2

            @pl.when(j < near)
            def _():
                fetch(phase, j + SLOTS // 2, side)

            if side == RIGHT:
                @pl.when(j == near)
                def _():
                    fetch(phase + 1, 0, RIGHT)

            @pl.when(j > near if side == RIGHT else j >= near)
            def _():
                fetch(phase + 1, 2 * (j - near) + side, RIGHT)
        else:
            near = chunks - SLOTS
            if isinstance(j, int):
                assert j < near
                fetch(phase, j + SLOTS, RIGHT)
                return

            @pl.when(j < near)
            def _():
                fetch(phase, j + SLOTS, RIGHT)

            if phase + 1 < len(split):
                for k in range(SLOTS):
                    @pl.when(j == near + k)
                    def _(k=k):
                        fetch(phase + 1, k // 2, k % 2)

    for side in (RIGHT, LEFT):
        for p in range(PIECES):
            for copy in piece_copies(side, p):
                copy.start()
    for side in (RIGHT, LEFT):
        g_load(matrix(0, side), 1, slot_of(0, 1, side))

    barrier = pltpu.get_barrier_semaphore()
    for side in (RIGHT, LEFT):
        pl.semaphore_signal(barrier, inc=1, device_id={axis: peer[side]}, device_id_type=pl.DeviceIdType.MESH)

    step = tokens // PIECES
    for side in (RIGHT, LEFT):
        term = None
        for p in range(PIECES):
            for copy in piece_copies(side, p):
                copy.wait()
            rows_p = pl.ds(p * step, step)
            part = product(a_buf[0, rows_p, half_rows(side)], g_buf[side, rows_p, pl.ds(0, narrow)])
            term = part if term is None else term + part
        if side == RIGHT:
            pl.semaphore_wait(barrier, 2)
        pass_on(0, side, 0, term)
        refill(0, 0, side)

    def block(phase, j):
        w = width(j)
        if split[phase]:
            for side in (RIGHT, LEFT):
                slot = slot_of(phase, j, side)
                g_wait(j, slot)
                term = product(a_buf[phase % 2, :, half_rows(side)], g_buf[slot, :, pl.ds(0, w)])
                pass_on(phase, side, j, term)
                refill(phase, j, side)
        else:
            slot = slot_of(phase, j, RIGHT)
            g_wait(j, slot)
            terms = product(a_buf[phase % 2], g_buf[slot, :, pl.ds(0, w)])
            for side in (RIGHT, LEFT):
                pass_on(phase, side, j, terms[side * half:(side + 1) * half])
            refill(phase, j, RIGHT)

    for phase in range(len(split)):
        if phase + 1 < len(split):
            for side in (RIGHT, LEFT):
                a_load(phase + 1, side)
        if phase > 0:
            for side in (RIGHT, LEFT):
                a_wait(phase, side)
            block(phase, 0)
        lax.fori_loop(1, chunks, lambda j, _, phase=phase: (block(phase, j), 0)[1], 0)

    last = 2 * (group - 1)
    for n in range(group - 1, last - 1):
        for j in range(chunks):
            for side in (RIGHT, LEFT):
                arrived(side, n, j).wait_recv()
                hop(side, n + 1, j).start()
    for j in range(chunks):
        for side in (RIGHT, LEFT):
            arrived(side, last - 1, j).wait_recv()
    for n in range(last):
        for j in range(chunks):
            for side in (RIGHT, LEFT):
                hop(side, n, j).wait_send()


def solution(mesh):
    axis = "dp"
    group = mesh.shape[axis]

    def sums(a, g):
        a, g = a.reshape(a.shape[1:]), g.reshape(g.shape[1:])
        matrices, tokens, rows = a.shape
        columns = g.shape[2]
        narrow = columns % WIDE or WIDE
        chunks = 1 + (columns - narrow) // WIDE
        half = rows // 2
        hops = 2 * (group - 1)
        return pl.pallas_call(
            functools.partial(kernel, axis, group),
            out_shape=pltpu.VMEM((matrices, rows, columns), a.dtype),
            in_specs=[pl.BlockSpec(memory_space=pltpu.HBM)] * 2,
            out_specs=pl.BlockSpec(memory_space=pltpu.VMEM),
            scratch_shapes=[
                pltpu.VMEM((2, tokens, rows), a.dtype),
                pltpu.VMEM((SLOTS, tokens, WIDE), a.dtype),
                pltpu.VMEM((2, chunks, half, WIDE), a.dtype),
                pltpu.VMEM((group - 1, 2, chunks, half, WIDE), a.dtype),
                pltpu.SemaphoreType.DMA((2, 2)),
                pltpu.SemaphoreType.DMA((2, PIECES)),
                pltpu.SemaphoreType.DMA((SLOTS,)),
                pltpu.SemaphoreType.DMA((2, PIECES)),
                pltpu.SemaphoreType.DMA((2, hops, chunks)),
                pltpu.SemaphoreType.DMA((2, hops, chunks)),
            ],
            compiler_params=pltpu.CompilerParams(
                collective_id=0, has_side_effects=True, vmem_limit_bytes=52 * 2**20
            ),
            cost_estimate=pl.CostEstimate(
                flops=2 * matrices * tokens * rows * columns,
                bytes_accessed=2 * matrices * tokens * (rows + columns),
                transcendentals=0,
            ),
            name="sums",
        )(a, g)

    spec = jax.P(("rep", axis))
    return jax.shard_map(sums, mesh=mesh, in_specs=(spec, spec), out_specs=jax.P("rep"), check_vma=False)
```

```python
import functools

import jax
import jax.numpy as jnp
from jax import lax
from jax.experimental import pallas as pl
from jax.experimental.pallas import tpu as pltpu

TILE = 128
WIDE = 2 * TILE
SLOTS = 4
PIECES = 4
RIGHT, LEFT = 0, 1
GROUP = 4
HOPS = 2 * (GROUP - 1)


def kernel(axis, a_hbm, g_hbm, out, a_buf, g_buf, terms, first, landed, a_sem, a0_sem, g_sem, g0_sem, send_sem, recv_sem):
    matrices, tokens, rows = a_hbm.shape
    columns = g_hbm.shape[2]
    half = rows // 2
    pairs = columns // WIDE
    wide_units = matrices * pairs // 2
    units = wide_units + 1
    blocks = matrices * (pairs + 1)
    cycle = 2 * (pairs + 1)
    me = lax.axis_index(axis)
    ring = [lax.rem(me + k, GROUP) for k in range(GROUP)]
    peer = (ring[1], ring[GROUP - 1])

    def half_rows(side):
        return pl.ds(side * half, half)

    def block_place(i):
        group, q = i // cycle, i % cycle
        narrow = q // (pairs + 1) - q // (pairs + 2) + q // (cycle - 1)
        r = q - q // (pairs + 2)
        unit, second = group * pairs + r // 2, r % 2
        pair = 2 * unit + second * (me % 2) + (1 - second) * (1 - me % 2)
        narrow_m = 2 * group + q // (cycle - 1)
        m = narrow * narrow_m + (1 - narrow) * (pair // pairs)
        column = narrow * (columns - WIDE) + (1 - narrow) * (pair % pairs) * WIDE
        kept = narrow * (2 * wide_units + narrow_m) + (1 - narrow) * (2 * unit + second)
        return m, pl.multiple_of(column, TILE), kept

    def g_load(i):
        m, column, _ = block_place(i)
        slot = i % SLOTS
        step = tokens // PIECES
        for p in range(PIECES):
            rows_p = pl.ds(p * step, step)
            pltpu.make_async_copy(
                g_hbm.at[m, rows_p, pl.ds(column, WIDE)], g_buf.at[slot, rows_p], g_sem.at[slot]
            ).start()

    def g_wait(i):
        slot = i % SLOTS
        pltpu.make_async_copy(g_hbm.at[0, :, pl.ds(0, WIDE)], g_buf.at[slot], g_sem.at[slot]).wait()

    def a_load(m):
        return pltpu.make_async_copy(a_hbm.at[m], a_buf.at[m % 2], a_sem.at[m % 2])

    def piece_copies(p):
        step = tokens // PIECES
        rows_p = pl.ds(p * step, step)
        m, column, _ = block_place(0)
        return (
            pltpu.make_async_copy(a_hbm.at[m, rows_p], a_buf.at[0, rows_p], a0_sem.at[p]),
            pltpu.make_async_copy(g_hbm.at[m, rows_p, pl.ds(column, WIDE)], g_buf.at[0, rows_p], g0_sem.at[p]),
        )

    def tile_place(u, owner):
        if isinstance(u, int) and u == wide_units:
            return owner, columns - TILE
        pair = 2 * u + owner % 2
        return pair // pairs, pl.multiple_of((pair % pairs) * WIDE + (owner // 2) * TILE, TILE)

    def term_of(u, k, side):
        owner = ring[k]
        if isinstance(u, int) and u == wide_units:
            return terms[2 * wide_units + owner, half_rows(side), pl.ds(TILE, TILE)]
        return terms[2 * u + 1 - k % 2, half_rows(side), pl.ds(pl.multiple_of((owner // 2) * TILE, TILE), TILE)]

    def out_tile(u, k, side):
        m, column = tile_place(u, ring[k])
        return out.at[m, half_rows(side), pl.ds(column, TILE)]

    def whose(side, n):
        k = (GROUP - 1 - n) % GROUP
        return k if side == RIGHT else (GROUP - k) % GROUP

    def remote(side, n, u, src, dst):
        return pltpu.make_async_remote_copy(
            src_ref=src,
            dst_ref=dst,
            send_sem=send_sem.at[side, n, u],
            recv_sem=recv_sem.at[side, n, u],
            device_id={axis: peer[side]},
            device_id_type=pl.DeviceIdType.MESH,
        )

    def hop(side, n, u):
        if n < GROUP - 1:
            return remote(side, n, u, first.at[side, u] if n == 0 else landed.at[n - 1, side, u], landed.at[n, side, u])
        tile = out_tile(u, whose(side, n), side)
        return remote(side, n, u, tile, tile)

    def arrival(side, n, u):
        if n < GROUP - 1:
            return hop(side, n, u)
        tile = out_tile(u, whose(side, n + 1), side)
        return remote(side, n, u, tile, tile)

    def send(n, u):
        for side in (RIGHT, LEFT):
            k = whose(side, n)
            if n == 0:
                first[side, u] = term_of(u, k, side).astype(first.dtype)
            else:
                arrival(side, n - 1, u).wait_recv()
                if n < GROUP:
                    total = (landed[n - 1, side, u].astype(jnp.float32) + term_of(u, k, side)).astype(first.dtype)
                    if n < GROUP - 1:
                        landed[n - 1, side, u] = total
                    else:
                        m, column = tile_place(u, me)
                        out[m, half_rows(side), pl.ds(column, TILE)] = total
            hop(side, n, u).start()

    def product(a, g):
        return lax.dot_general(a, g, (((0,), (0,)), ((), ())), preferred_element_type=jnp.float32)

    for p in range(PIECES):
        for copy in piece_copies(p):
            copy.start()
    for i in range(1, SLOTS):
        g_load(i)
    a_load(1).start()

    barrier = pltpu.get_barrier_semaphore()
    for side in (RIGHT, LEFT):
        pl.semaphore_signal(barrier, inc=1, device_id={axis: peer[side]}, device_id_type=pl.DeviceIdType.MESH)

    step = tokens // PIECES
    term = None
    for p in range(PIECES):
        for copy in piece_copies(p):
            copy.wait()
        part = product(a_buf[0, pl.ds(p * step, step)], g_buf[0, pl.ds(p * step, step)])
        term = part if term is None else term + part
    terms[0] = term
    g_load(SLOTS)
    pl.semaphore_wait(barrier, 2)
    send(0, 0)

    def body(i, _):
        m, _, kept = block_place(i)
        group, q = i // cycle, i % cycle
        @pl.when(i == pairs - 1)
        def _():
            a_load(1).wait()

        @pl.when(i == cycle)
        def _():
            a_load(2).wait()

        @pl.when(i == cycle + pairs - 1)
        def _():
            a_load(3).wait()

        g_wait(i)
        terms[kept] = product(a_buf[m % 2], g_buf[i % SLOTS])

        @pl.when(i + SLOTS < blocks)
        def _():
            g_load(i + SLOTS)

        @pl.when(i == pairs + 1)
        def _():
            a_load(2).start()

        @pl.when(i == cycle - 1)
        def _():
            a_load(3).start()

        narrow = q // (pairs + 1) - q // (pairs + 2) + q // (cycle - 1)
        r = q - q // (pairs + 2)
        u, second = group * pairs + r // 2, r % 2
        kind = 2 * narrow + second

        @pl.when(kind == 0)
        def _():
            send(0, u)

            @pl.when(u >= 1)
            def _():
                send(1, u - 1)

        @pl.when((kind == 1) & (u >= 2))
        def _():
            send(2, u - 2)

            @pl.when(u >= 3)
            def _():
                send(3, u - 3)

        return 0

    lax.fori_loop(1, blocks, body, 0)

    last = wide_units
    late = [(0, last), (1, last - 1), (2, last - 2), (3, last - 3), None,
            (1, last), (2, last - 1), (3, last - 2), None,
            (2, last), (3, last - 1), None, (3, last), None]
    fill = [(4, u) for u in range(units - 3)] + [(5, u) for u in range(3)]
    for item in late:
        if item is not None:
            send(*item)
        else:
            for _ in range(3):
                if fill:
                    send(*fill.pop(0))
    for item in fill:
        send(*item)
    for u in range(units - 3, units):
        send(4, u)
    for u in range(3, units):
        send(5, u)
    for u in range(units):
        for side in (RIGHT, LEFT):
            arrival(side, HOPS - 1, u).wait_recv()
    for n in range(HOPS):
        for u in range(units):
            for side in (RIGHT, LEFT):
                hop(side, n, u).wait_send()


def solution(mesh):
    axis = "dp"

    def sums(a, g):
        a, g = a.reshape(a.shape[1:]), g.reshape(g.shape[1:])
        matrices, tokens, rows = a.shape
        columns = g.shape[2]
        pairs = columns // WIDE
        units = matrices * pairs // 2 + 1
        half = rows // 2
        assert mesh.shape[axis] == GROUP == matrices and columns % WIDE == TILE
        return pl.pallas_call(
            functools.partial(kernel, axis),
            out_shape=pltpu.VMEM((matrices, rows, columns), a.dtype),
            in_specs=[pl.BlockSpec(memory_space=pltpu.HBM)] * 2,
            out_specs=pl.BlockSpec(memory_space=pltpu.VMEM),
            scratch_shapes=[
                pltpu.VMEM((2, tokens, rows), a.dtype),
                pltpu.VMEM((SLOTS, tokens, WIDE), a.dtype),
                pltpu.VMEM((matrices * (pairs + 1), rows, WIDE), jnp.float32),
                pltpu.VMEM((2, units, half, TILE), a.dtype),
                pltpu.VMEM((GROUP - 1, 2, units, half, TILE), a.dtype),
                pltpu.SemaphoreType.DMA((2,)),
                pltpu.SemaphoreType.DMA((PIECES,)),
                pltpu.SemaphoreType.DMA((SLOTS,)),
                pltpu.SemaphoreType.DMA((PIECES,)),
                pltpu.SemaphoreType.DMA((2, HOPS, units)),
                pltpu.SemaphoreType.DMA((2, HOPS, units)),
            ],
            compiler_params=pltpu.CompilerParams(
                collective_id=0, has_side_effects=True, vmem_limit_bytes=57 * 2**20
            ),
            cost_estimate=pl.CostEstimate(
                flops=2 * matrices * tokens * rows * columns,
                bytes_accessed=2 * matrices * tokens * (rows + columns),
                transcendentals=0,
            ),
            name="sums",
        )(a, g)

    spec = jax.P(("rep", axis))
    return jax.shard_map(sums, mesh=mesh, in_specs=(spec, spec), out_specs=jax.P("rep"), check_vma=False)
```

```python
import functools

import jax
import jax.numpy as jnp
from jax import lax
from jax.experimental import pallas as pl
from jax.experimental.pallas import tpu as pltpu

TILE = 128
WIDE = 2 * TILE
SLOTS = 4
PIECES = 4
RIGHT, LEFT = 0, 1
GROUP = 4
HOPS = 2 * (GROUP - 1)
SENDS = (
    ((0, 0),),
    ((0, 1),),
    ((1, 0),),
    ((1, 1),),
    ((0, 2), (2, 0)),
    ((2, 1),),
    ((1, 2), (3, 0)),
    ((0, 3), (3, 1)),
    ((2, 2), (4, 0)),
    ((0, 4), (1, 3), (4, 1)),
    ((3, 2), (5, 0)),
    ((1, 4), (2, 3)),
    ((0, 5), (4, 2), (5, 1)),
    ((0, 6), (2, 4)),
    ((1, 5), (3, 3)),
    ((1, 6), (5, 2)),
    ((0, 7), (2, 5), (3, 4)),
    ((2, 6), (4, 3)),
    ((1, 7), (3, 5)),
    ((0, 8), (3, 6)),
    ((2, 7), (4, 4)),
    ((0, 9), (1, 8), (4, 5)),
    ((3, 7), (4, 6)),
    ((0, 10), (1, 9)),
)
LATE = (
    (2, 8), (1, 10), (2, 9), (3, 8), (2, 10), (3, 9), (4, 7), (3, 10),
    (4, 8), (4, 9), (4, 10), (5, 3), (5, 4), (5, 5), (5, 6), (5, 7),
    (5, 8), (5, 9), (5, 10),
)


def kernel(axis, a_hbm, g_hbm, out, a_buf, g_buf, terms, first, landed, a_sem, a0_sem, g_sem, g0_sem, send_sem, recv_sem):
    matrices, tokens, rows = a_hbm.shape
    columns = g_hbm.shape[2]
    half = rows // 2
    pairs = columns // WIDE
    wide_units = matrices * pairs // 2
    units = wide_units + 1
    blocks = matrices * (pairs + 1)
    cycle = 2 * (pairs + 1)
    me = lax.axis_index(axis)
    ring = [lax.rem(me + k, GROUP) for k in range(GROUP)]
    peer = (ring[1], ring[GROUP - 1])

    def half_rows(side):
        return pl.ds(side * half, half)

    def block_place(i):
        group, q = i // cycle, i % cycle
        narrow = q // (pairs + 1) - q // (pairs + 2) + q // (cycle - 1)
        r = q - q // (pairs + 2)
        swap = (r + cycle - 1) // cycle - (r + cycle - 3) // cycle
        r = swap * (3 - r) + (1 - swap) * r
        unit, second = group * pairs + r // 2, r % 2
        pair = 2 * unit + second * (me % 2) + (1 - second) * (1 - me % 2)
        narrow_m = 2 * group + q // (cycle - 1)
        m = narrow * narrow_m + (1 - narrow) * (pair // pairs)
        column = narrow * (columns - WIDE) + (1 - narrow) * (pair % pairs) * WIDE
        kept = narrow * (2 * wide_units + narrow_m) + (1 - narrow) * (2 * unit + second)
        return m, pl.multiple_of(column, TILE), kept

    def g_load(i):
        m, column, _ = block_place(i)
        slot = i % SLOTS
        step = tokens // PIECES
        for p in range(PIECES):
            rows_p = pl.ds(p * step, step)
            pltpu.make_async_copy(
                g_hbm.at[m, rows_p, pl.ds(column, WIDE)], g_buf.at[slot, rows_p], g_sem.at[slot]
            ).start()

    def g_wait(i):
        slot = i % SLOTS
        pltpu.make_async_copy(g_hbm.at[0, :, pl.ds(0, WIDE)], g_buf.at[slot], g_sem.at[slot]).wait()

    def a_load(m):
        return pltpu.make_async_copy(a_hbm.at[m], a_buf.at[m % 2], a_sem.at[m % 2])

    def piece_copies(p):
        step = tokens // PIECES
        rows_p = pl.ds(p * step, step)
        m, column, _ = block_place(0)
        return (
            pltpu.make_async_copy(a_hbm.at[m, rows_p], a_buf.at[0, rows_p], a0_sem.at[p]),
            pltpu.make_async_copy(g_hbm.at[m, rows_p, pl.ds(column, WIDE)], g_buf.at[0, rows_p], g0_sem.at[p]),
        )

    def tile_place(u, owner):
        if isinstance(u, int) and u == wide_units:
            return owner, columns - TILE
        pair = 2 * u + owner % 2
        return pair // pairs, pl.multiple_of((pair % pairs) * WIDE + (owner // 2) * TILE, TILE)

    def term_of(u, k, side):
        owner = ring[k]
        if isinstance(u, int) and u == wide_units:
            return terms[2 * wide_units + owner, half_rows(side), pl.ds(TILE, TILE)]
        return terms[2 * u + 1 - k % 2, half_rows(side), pl.ds(pl.multiple_of((owner // 2) * TILE, TILE), TILE)]

    def out_tile(u, k, side):
        m, column = tile_place(u, ring[k])
        return out.at[m, half_rows(side), pl.ds(column, TILE)]

    def whose(side, n):
        k = (GROUP - 1 - n) % GROUP
        return k if side == RIGHT else (GROUP - k) % GROUP

    def remote(side, n, u, src, dst):
        return pltpu.make_async_remote_copy(
            src_ref=src,
            dst_ref=dst,
            send_sem=send_sem.at[side, n, u],
            recv_sem=recv_sem.at[side, n, u],
            device_id={axis: peer[side]},
            device_id_type=pl.DeviceIdType.MESH,
        )

    def hop(side, n, u):
        if n < GROUP - 1:
            return remote(side, n, u, first.at[side, u] if n == 0 else landed.at[n - 1, side, u], landed.at[n, side, u])
        tile = out_tile(u, whose(side, n), side)
        return remote(side, n, u, tile, tile)

    def arrival(side, n, u):
        if n < GROUP - 1:
            return hop(side, n, u)
        tile = out_tile(u, whose(side, n + 1), side)
        return remote(side, n, u, tile, tile)

    def send(n, u):
        for side in (RIGHT, LEFT):
            k = whose(side, n)
            if n == 0:
                first[side, u] = term_of(u, k, side).astype(first.dtype)
            else:
                arrival(side, n - 1, u).wait_recv()
                if n < GROUP:
                    total = (landed[n - 1, side, u].astype(jnp.float32) + term_of(u, k, side)).astype(first.dtype)
                    if n < GROUP - 1:
                        landed[n - 1, side, u] = total
                    else:
                        m, column = tile_place(u, me)
                        out[m, half_rows(side), pl.ds(column, TILE)] = total
            hop(side, n, u).start()

    def product(a, g):
        return lax.dot_general(a, g, (((0,), (0,)), ((), ())), preferred_element_type=jnp.float32)

    for p in range(PIECES):
        for copy in piece_copies(p):
            copy.start()
    for i in range(1, SLOTS):
        g_load(i)
    a_load(1).start()

    barrier = pltpu.get_barrier_semaphore()
    for side in (RIGHT, LEFT):
        pl.semaphore_signal(barrier, inc=1, device_id={axis: peer[side]}, device_id_type=pl.DeviceIdType.MESH)

    step = tokens // PIECES
    term = None
    for p in range(PIECES):
        for copy in piece_copies(p):
            copy.wait()
        part = product(a_buf[0, pl.ds(p * step, step)], g_buf[0, pl.ds(p * step, step)])
        term = part if term is None else term + part
    terms[0] = term
    g_load(SLOTS)
    pl.semaphore_wait(barrier, 2)
    send(0, 0)

    def body(i, _):
        m, _, kept = block_place(i)
        @pl.when(i == pairs - 1)
        def _():
            a_load(1).wait()

        @pl.when(i == cycle)
        def _():
            a_load(2).wait()

        @pl.when(i == cycle + pairs - 1)
        def _():
            a_load(3).wait()

        g_wait(i)
        terms[kept] = product(a_buf[m % 2], g_buf[i % SLOTS])

        @pl.when(i + SLOTS < blocks)
        def _():
            g_load(i + SLOTS)

        @pl.when(i == pairs + 1)
        def _():
            a_load(2).start()

        @pl.when(i == cycle - 1)
        def _():
            a_load(3).start()

        for k in range(1, blocks):
            if SENDS[k]:
                @pl.when(i == k)
                def _(k=k):
                    for n, u in SENDS[k]:
                        send(n, u)

        return 0

    lax.fori_loop(1, blocks, body, 0)

    for n, u in LATE:
        send(n, u)
    for u in range(units):
        for side in (RIGHT, LEFT):
            arrival(side, HOPS - 1, u).wait_recv()
    for n in range(HOPS):
        for u in range(units):
            for side in (RIGHT, LEFT):
                hop(side, n, u).wait_send()


def solution(mesh):
    axis = "dp"

    def sums(a, g):
        a, g = a.reshape(a.shape[1:]), g.reshape(g.shape[1:])
        matrices, tokens, rows = a.shape
        columns = g.shape[2]
        pairs = columns // WIDE
        units = matrices * pairs // 2 + 1
        half = rows // 2
        assert mesh.shape[axis] == GROUP == matrices and columns % WIDE == TILE
        return pl.pallas_call(
            functools.partial(kernel, axis),
            out_shape=pltpu.VMEM((matrices, rows, columns), a.dtype),
            in_specs=[pl.BlockSpec(memory_space=pltpu.HBM)] * 2,
            out_specs=pl.BlockSpec(memory_space=pltpu.VMEM),
            scratch_shapes=[
                pltpu.VMEM((2, tokens, rows), a.dtype),
                pltpu.VMEM((SLOTS, tokens, WIDE), a.dtype),
                pltpu.VMEM((matrices * (pairs + 1), rows, WIDE), jnp.float32),
                pltpu.VMEM((2, units, half, TILE), a.dtype),
                pltpu.VMEM((GROUP - 1, 2, units, half, TILE), a.dtype),
                pltpu.SemaphoreType.DMA((2,)),
                pltpu.SemaphoreType.DMA((PIECES,)),
                pltpu.SemaphoreType.DMA((SLOTS,)),
                pltpu.SemaphoreType.DMA((PIECES,)),
                pltpu.SemaphoreType.DMA((2, HOPS, units)),
                pltpu.SemaphoreType.DMA((2, HOPS, units)),
            ],
            compiler_params=pltpu.CompilerParams(
                collective_id=0, has_side_effects=True, vmem_limit_bytes=57 * 2**20
            ),
            cost_estimate=pl.CostEstimate(
                flops=2 * matrices * tokens * rows * columns,
                bytes_accessed=2 * matrices * tokens * (rows + columns),
                transcendentals=0,
            ),
            name="sums",
        )(a, g)

    spec = jax.P(("rep", axis))
    return jax.shard_map(sums, mesh=mesh, in_specs=(spec, spec), out_specs=jax.P("rep"), check_vma=False)
```

```python
import functools

import jax
import jax.numpy as jnp
from jax import lax
from jax.experimental import pallas as pl
from jax.experimental.pallas import tpu as pltpu

TILE = 128
WIDE = 2 * TILE
SLOTS = 4
PIECES = 4
OPENING = 8
RIGHT, LEFT = 0, 1
GROUP = 4
HOPS = 2 * (GROUP - 1)
SENDS = (
    ((0, 0),),
    ((0, 1),),
    ((1, 0),),
    ((1, 1),),
    ((0, 2), (2, 0)),
    ((2, 1),),
    ((1, 2), (3, 0)),
    ((0, 3), (3, 1)),
    ((2, 2), (4, 0)),
    ((0, 4), (1, 3), (4, 1)),
    ((3, 2), (5, 0)),
    ((1, 4), (2, 3)),
    ((0, 5), (4, 2), (5, 1)),
    ((0, 6), (2, 4)),
    ((1, 5), (3, 3), (5, 2)),
    ((1, 6),),
    ((0, 7), (2, 5), (3, 4)),
    ((4, 3),),
    ((1, 7), (2, 6)),
    ((0, 8), (3, 5), (4, 4)),
    ((2, 7), (5, 3), (3, 6)),
    ((0, 9), (1, 8)),
    ((3, 7), (4, 5)),
    ((0, 10), (4, 6)),
)
LATE = (
    (1, 9), (2, 8), (1, 10), (4, 7), (2, 9), (3, 8), (2, 10), (5, 4),
    (3, 9), (4, 8), (3, 10), (5, 5), (4, 9), (5, 6), (4, 10), (5, 7),
    (5, 8), (5, 9), (5, 10),
)


def kernel(axis, a_hbm, g_hbm, out, a_buf, g_buf, terms, first, landed, a_sem, a0_sem, g_sem, g0_sem, send_sem, recv_sem):
    matrices, tokens, rows = a_hbm.shape
    columns = g_hbm.shape[2]
    half = rows // 2
    pairs = columns // WIDE
    wide_units = matrices * pairs // 2
    units = wide_units + 1
    blocks = matrices * (pairs + 1)
    cycle = 2 * (pairs + 1)
    me = lax.axis_index(axis)
    ring = [lax.rem(me + k, GROUP) for k in range(GROUP)]
    peer = (ring[1], ring[GROUP - 1])

    def half_rows(side):
        return pl.ds(side * half, half)

    def block_place(i):
        group, q = i // cycle, i % cycle
        narrow = q // (pairs + 1) - q // (pairs + 2) + q // (cycle - 1)
        r = q - q // (pairs + 2)
        swap = (r + cycle - 1) // cycle - (r + cycle - 3) // cycle
        r = swap * (3 - r) + (1 - swap) * r
        unit, second = group * pairs + r // 2, r % 2
        pair = 2 * unit + second * (me % 2) + (1 - second) * (1 - me % 2)
        narrow_m = 2 * group + q // (cycle - 1)
        m = narrow * narrow_m + (1 - narrow) * (pair // pairs)
        column = narrow * (columns - WIDE) + (1 - narrow) * (pair % pairs) * WIDE
        kept = narrow * (2 * wide_units + narrow_m) + (1 - narrow) * (2 * unit + second)
        return m, pl.multiple_of(column, TILE), kept

    def g_load(i):
        m, column, _ = block_place(i)
        slot = i % SLOTS
        step = tokens // PIECES
        for p in range(PIECES):
            rows_p = pl.ds(p * step, step)
            pltpu.make_async_copy(
                g_hbm.at[m, rows_p, pl.ds(column, WIDE)], g_buf.at[slot, rows_p], g_sem.at[slot]
            ).start()

    def g_wait(i):
        slot = i % SLOTS
        pltpu.make_async_copy(g_hbm.at[0, :, pl.ds(0, WIDE)], g_buf.at[slot], g_sem.at[slot]).wait()

    def a_load(m):
        return pltpu.make_async_copy(a_hbm.at[m], a_buf.at[m % 2], a_sem.at[m % 2])

    def piece_copies(p):
        step = tokens // OPENING
        rows_p = pl.ds(p * step, step)
        m, column, _ = block_place(0)
        return (
            pltpu.make_async_copy(a_hbm.at[m, rows_p], a_buf.at[0, rows_p], a0_sem.at[p]),
            pltpu.make_async_copy(g_hbm.at[m, rows_p, pl.ds(column, WIDE)], g_buf.at[0, rows_p], g0_sem.at[p]),
        )

    def tile_place(u, owner):
        if isinstance(u, int) and u == wide_units:
            return owner, columns - TILE
        pair = 2 * u + owner % 2
        return pair // pairs, pl.multiple_of((pair % pairs) * WIDE + (owner // 2) * TILE, TILE)

    def term_of(u, k, side):
        owner = ring[k]
        if isinstance(u, int) and u == wide_units:
            return terms[2 * wide_units + owner, half_rows(side), pl.ds(TILE, TILE)]
        return terms[2 * u + 1 - k % 2, half_rows(side), pl.ds(pl.multiple_of((owner // 2) * TILE, TILE), TILE)]

    def out_tile(u, k, side):
        m, column = tile_place(u, ring[k])
        return out.at[m, half_rows(side), pl.ds(column, TILE)]

    def whose(side, n):
        k = (GROUP - 1 - n) % GROUP
        return k if side == RIGHT else (GROUP - k) % GROUP

    def remote(side, n, u, src, dst):
        return pltpu.make_async_remote_copy(
            src_ref=src,
            dst_ref=dst,
            send_sem=send_sem.at[side, n, u],
            recv_sem=recv_sem.at[side, n, u],
            device_id={axis: peer[side]},
            device_id_type=pl.DeviceIdType.MESH,
        )

    def hop(side, n, u):
        if n < GROUP - 1:
            return remote(side, n, u, first.at[side, u] if n == 0 else landed.at[n - 1, side, u], landed.at[n, side, u])
        tile = out_tile(u, whose(side, n), side)
        return remote(side, n, u, tile, tile)

    def arrival(side, n, u):
        if n < GROUP - 1:
            return hop(side, n, u)
        tile = out_tile(u, whose(side, n + 1), side)
        return remote(side, n, u, tile, tile)

    def send(n, u):
        for side in (RIGHT, LEFT):
            if n > 0:
                arrival(side, n - 1, u).wait_recv()
        for side in (RIGHT, LEFT):
            k = whose(side, n)
            if n == 0:
                first[side, u] = term_of(u, k, side).astype(first.dtype)
            elif n < GROUP:
                total = (landed[n - 1, side, u].astype(jnp.float32) + term_of(u, k, side)).astype(first.dtype)
                if n < GROUP - 1:
                    landed[n - 1, side, u] = total
                else:
                    m, column = tile_place(u, me)
                    out[m, half_rows(side), pl.ds(column, TILE)] = total
        for side in (RIGHT, LEFT):
            hop(side, n, u).start()

    def product(a, g):
        return lax.dot_general(a, g, (((0,), (0,)), ((), ())), preferred_element_type=jnp.float32)

    for p in range(OPENING):
        for copy in piece_copies(p):
            copy.start()
    for i in range(1, SLOTS):
        g_load(i)
    a_load(1).start()

    barrier = pltpu.get_barrier_semaphore()
    for side in (RIGHT, LEFT):
        pl.semaphore_signal(barrier, inc=1, device_id={axis: peer[side]}, device_id_type=pl.DeviceIdType.MESH)

    step = tokens // OPENING
    term = None
    for p in range(OPENING):
        for copy in piece_copies(p):
            copy.wait()
        part = product(a_buf[0, pl.ds(p * step, step)], g_buf[0, pl.ds(p * step, step)])
        term = part if term is None else term + part
    terms[0] = term
    g_load(SLOTS)
    pl.semaphore_wait(barrier, 2)
    send(0, 0)

    def body(i, _):
        m, _, kept = block_place(i)
        @pl.when(i == pairs - 1)
        def _():
            a_load(1).wait()

        @pl.when(i == cycle)
        def _():
            a_load(2).wait()

        @pl.when(i == cycle + pairs - 1)
        def _():
            a_load(3).wait()

        g_wait(i)
        terms[kept] = product(a_buf[m % 2], g_buf[i % SLOTS])

        @pl.when(i + SLOTS < blocks)
        def _():
            g_load(i + SLOTS)

        @pl.when(i == pairs + 1)
        def _():
            a_load(2).start()

        @pl.when(i == cycle - 1)
        def _():
            a_load(3).start()

        for k in range(1, blocks):
            if SENDS[k]:
                @pl.when(i == k)
                def _(k=k):
                    for n, u in SENDS[k]:
                        send(n, u)

        return 0

    lax.fori_loop(1, blocks, body, 0)

    for n, u in LATE:
        send(n, u)
    for u in range(units):
        for side in (RIGHT, LEFT):
            arrival(side, HOPS - 1, u).wait_recv()
    for n in range(HOPS):
        for u in range(units):
            for side in (RIGHT, LEFT):
                hop(side, n, u).wait_send()


def solution(mesh):
    axis = "dp"

    def sums(a, g):
        a, g = a.reshape(a.shape[1:]), g.reshape(g.shape[1:])
        matrices, tokens, rows = a.shape
        columns = g.shape[2]
        pairs = columns // WIDE
        units = matrices * pairs // 2 + 1
        half = rows // 2
        assert mesh.shape[axis] == GROUP == matrices and columns % WIDE == TILE
        return pl.pallas_call(
            functools.partial(kernel, axis),
            out_shape=pltpu.VMEM((matrices, rows, columns), a.dtype),
            in_specs=[pl.BlockSpec(memory_space=pltpu.HBM)] * 2,
            out_specs=pl.BlockSpec(memory_space=pltpu.VMEM),
            scratch_shapes=[
                pltpu.VMEM((2, tokens, rows), a.dtype),
                pltpu.VMEM((SLOTS, tokens, WIDE), a.dtype),
                pltpu.VMEM((matrices * (pairs + 1), rows, WIDE), jnp.float32),
                pltpu.VMEM((2, units, half, TILE), a.dtype),
                pltpu.VMEM((GROUP - 1, 2, units, half, TILE), a.dtype),
                pltpu.SemaphoreType.DMA((2,)),
                pltpu.SemaphoreType.DMA((OPENING,)),
                pltpu.SemaphoreType.DMA((SLOTS,)),
                pltpu.SemaphoreType.DMA((OPENING,)),
                pltpu.SemaphoreType.DMA((2, HOPS, units)),
                pltpu.SemaphoreType.DMA((2, HOPS, units)),
            ],
            compiler_params=pltpu.CompilerParams(
                collective_id=0, has_side_effects=True, vmem_limit_bytes=57 * 2**20
            ),
            cost_estimate=pl.CostEstimate(
                flops=2 * matrices * tokens * rows * columns,
                bytes_accessed=2 * matrices * tokens * (rows + columns),
                transcendentals=0,
            ),
            name="sums",
        )(a, g)

    spec = jax.P(("rep", axis))
    return jax.shard_map(sums, mesh=mesh, in_specs=(spec, spec), out_specs=jax.P("rep"), check_vma=False)
```

```python
import functools

import jax
import jax.numpy as jnp
from jax import lax
from jax.experimental import pallas as pl
from jax.experimental.pallas import tpu as pltpu

TILE = 128
WIDE = 2 * TILE
SLOTS = 4
PIECES = 4
OPENING = 8
RIGHT, LEFT = 0, 1
GROUP = 4
HOPS = 2 * (GROUP - 1)
SENDS = (
    ((0, 0),),
    ((0, 1),),
    ((1, 0),),
    ((1, 1),),
    ((0, 2), (2, 0)),
    ((2, 1),),
    ((1, 2), (3, 0)),
    ((0, 3), (3, 1)),
    ((2, 2), (4, 0)),
    ((0, 4), (1, 3), (4, 1)),
    ((3, 2), (5, 0)),
    ((1, 4), (2, 3)),
    ((0, 5), (4, 2), (5, 1)),
    ((0, 6), (2, 4)),
    ((1, 5), (3, 3), (5, 2)),
    ((1, 6),),
    ((0, 7), (2, 5), (3, 4)),
    ((4, 3),),
    ((1, 7), (2, 6)),
    ((0, 8), (3, 5), (4, 4)),
    ((2, 7), (5, 3), (3, 6)),
    ((0, 9), (1, 8)),
    ((3, 7), (4, 5)),
    ((0, 10), (4, 6)),
)
LATE = (
    (1, 9), (2, 8), (1, 10), (4, 7), (2, 9), (3, 8), (2, 10), (5, 4),
    (3, 9), (4, 8), (3, 10), (5, 5), (4, 9), (5, 6), (4, 10), (5, 7),
    (5, 8), (5, 9), (5, 10),
)


def kernel(axis, a_hbm, g_hbm, out, a_buf, g_buf, terms, first, landed, a_sem, a0_sem, g_sem, g0_sem, send_sem, recv_sem):
    matrices, tokens, rows = a_hbm.shape
    columns = g_hbm.shape[2]
    half = rows // 2
    pairs = columns // WIDE
    wide_units = matrices * pairs // 2
    units = wide_units + 1
    blocks = matrices * (pairs + 1)
    cycle = 2 * (pairs + 1)
    me = lax.axis_index(axis)
    ring = [lax.rem(me + k, GROUP) for k in range(GROUP)]
    peer = (ring[1], ring[GROUP - 1])

    def half_rows(side):
        return pl.ds(side * half, half)

    def block_place(i):
        group, q = i // cycle, i % cycle
        narrow = q // (pairs + 1) - q // (pairs + 2) + q // (cycle - 1)
        r = q - q // (pairs + 2)
        swap = (r + cycle - 1) // cycle - (r + cycle - 3) // cycle
        r = swap * (3 - r) + (1 - swap) * r
        unit, second = group * pairs + r // 2, r % 2
        pair = 2 * unit + second * (me % 2) + (1 - second) * (1 - me % 2)
        narrow_m = 2 * group + q // (cycle - 1)
        m = narrow * narrow_m + (1 - narrow) * (pair // pairs)
        column = narrow * (columns - WIDE) + (1 - narrow) * (pair % pairs) * WIDE
        kept = narrow * (2 * wide_units + narrow_m) + (1 - narrow) * (2 * unit + second)
        return m, pl.multiple_of(column, TILE), kept

    def g_load(i):
        m, column, _ = block_place(i)
        slot = i % SLOTS
        step = tokens // PIECES
        for p in range(PIECES):
            rows_p = pl.ds(p * step, step)
            pltpu.make_async_copy(
                g_hbm.at[m, rows_p, pl.ds(column, WIDE)], g_buf.at[slot, rows_p], g_sem.at[slot]
            ).start()

    def g_wait(i):
        slot = i % SLOTS
        pltpu.make_async_copy(g_hbm.at[0, :, pl.ds(0, WIDE)], g_buf.at[slot], g_sem.at[slot]).wait()

    def a_load(m):
        return pltpu.make_async_copy(a_hbm.at[m], a_buf.at[m % 2], a_sem.at[m % 2])

    def piece_copies(p):
        step = tokens // OPENING
        rows_p = pl.ds(p * step, step)
        m, column, _ = block_place(0)
        return (
            pltpu.make_async_copy(a_hbm.at[m, rows_p], a_buf.at[0, rows_p], a0_sem.at[p]),
            pltpu.make_async_copy(g_hbm.at[m, rows_p, pl.ds(column, WIDE)], g_buf.at[0, rows_p], g0_sem.at[p]),
        )

    def tile_place(u, owner):
        if isinstance(u, int) and u == wide_units:
            return owner, columns - TILE
        pair = 2 * u + owner % 2
        return pair // pairs, pl.multiple_of((pair % pairs) * WIDE + (owner // 2) * TILE, TILE)

    def term_of(u, k, side):
        owner = ring[k]
        if isinstance(u, int) and u == wide_units:
            return terms[2 * wide_units + owner, half_rows(side), pl.ds(TILE, TILE)]
        return terms[2 * u + 1 - k % 2, half_rows(side), pl.ds(pl.multiple_of((owner // 2) * TILE, TILE), TILE)]

    def out_tile(u, k, side):
        m, column = tile_place(u, ring[k])
        return out.at[m, half_rows(side), pl.ds(column, TILE)]

    def whose(side, n):
        k = (GROUP - 1 - n) % GROUP
        return k if side == RIGHT else (GROUP - k) % GROUP

    def remote(side, n, u, src, dst):
        return pltpu.make_async_remote_copy(
            src_ref=src,
            dst_ref=dst,
            send_sem=send_sem.at[side, n, u],
            recv_sem=recv_sem.at[side, n, u],
            device_id={axis: peer[side]},
            device_id_type=pl.DeviceIdType.MESH,
        )

    def hop(side, n, u):
        if n < GROUP - 1:
            return remote(side, n, u, first.at[side, u] if n == 0 else landed.at[n - 1, side, u], landed.at[n, side, u])
        tile = out_tile(u, whose(side, n), side)
        return remote(side, n, u, tile, tile)

    def arrival(side, n, u):
        if n < GROUP - 1:
            return hop(side, n, u)
        tile = out_tile(u, whose(side, n + 1), side)
        return remote(side, n, u, tile, tile)

    def send(n, u):
        for side in (RIGHT, LEFT):
            if n > 0:
                arrival(side, n - 1, u).wait_recv()
        for side in (RIGHT, LEFT):
            k = whose(side, n)
            if n == 0:
                first[side, u] = term_of(u, k, side).astype(first.dtype)
            elif n < GROUP:
                total = (landed[n - 1, side, u].astype(jnp.float32) + term_of(u, k, side)).astype(first.dtype)
                if n < GROUP - 1:
                    landed[n - 1, side, u] = total
                else:
                    m, column = tile_place(u, me)
                    out[m, half_rows(side), pl.ds(column, TILE)] = total
        for side in (RIGHT, LEFT):
            hop(side, n, u).start()

    def product(a, g):
        return lax.dot_general(a, g, (((0,), (0,)), ((), ())), preferred_element_type=jnp.float32)

    for p in range(OPENING):
        for copy in piece_copies(p):
            copy.start()
    for i in range(1, SLOTS):
        g_load(i)
    a_load(1).start()

    barrier = pltpu.get_barrier_semaphore()
    for side in (RIGHT, LEFT):
        pl.semaphore_signal(barrier, inc=1, device_id={axis: peer[side]}, device_id_type=pl.DeviceIdType.MESH)

    step = tokens // OPENING
    term = None
    for p in range(OPENING):
        for copy in piece_copies(p):
            copy.wait()
        part = product(a_buf[0, pl.ds(p * step, step)], g_buf[0, pl.ds(p * step, step)])
        term = part if term is None else term + part
    terms[0] = term
    g_load(SLOTS)
    pl.semaphore_wait(barrier, 2)
    send(0, 0)

    def body(i, _):
        m, _, kept = block_place(i)
        @pl.when(i == pairs - 1)
        def _():
            a_load(1).wait()

        @pl.when(i == cycle)
        def _():
            a_load(2).wait()

        @pl.when(i == cycle + pairs - 1)
        def _():
            a_load(3).wait()

        g_wait(i)
        q = i % cycle
        narrow = q // (pairs + 1) - q // (pairs + 2) + q // (cycle - 1)

        @pl.when(narrow == 0)
        def _():
            terms[kept] = product(a_buf[m % 2], g_buf[i % SLOTS])

        @pl.when(narrow == 1)
        def _():
            terms[kept, :, TILE:] = product(g_buf[i % SLOTS, :, TILE:], a_buf[m % 2]).T

        @pl.when(i + SLOTS < blocks)
        def _():
            g_load(i + SLOTS)

        @pl.when(i == pairs + 1)
        def _():
            a_load(2).start()

        @pl.when(i == cycle - 1)
        def _():
            a_load(3).start()

        for c in range(0, blocks, 5):
            @pl.when(i // 5 == c // 5)
            def _(c=c):
                for k in range(max(c, 1), min(c + 5, blocks)):
                    @pl.when(i == k)
                    def _(k=k):
                        for n, u in SENDS[k]:
                            send(n, u)

        return 0

    lax.fori_loop(1, blocks, body, 0)

    for n, u in LATE:
        send(n, u)
    for u in range(units):
        for side in (RIGHT, LEFT):
            arrival(side, HOPS - 1, u).wait_recv()
    for n in range(HOPS):
        for u in range(units):
            for side in (RIGHT, LEFT):
                hop(side, n, u).wait_send()


def solution(mesh):
    axis = "dp"

    def sums(a, g):
        a, g = a.reshape(a.shape[1:]), g.reshape(g.shape[1:])
        matrices, tokens, rows = a.shape
        columns = g.shape[2]
        pairs = columns // WIDE
        units = matrices * pairs // 2 + 1
        half = rows // 2
        assert mesh.shape[axis] == GROUP == matrices and columns % WIDE == TILE
        return pl.pallas_call(
            functools.partial(kernel, axis),
            out_shape=pltpu.VMEM((matrices, rows, columns), a.dtype),
            in_specs=[pl.BlockSpec(memory_space=pltpu.HBM)] * 2,
            out_specs=pl.BlockSpec(memory_space=pltpu.VMEM),
            scratch_shapes=[
                pltpu.VMEM((2, tokens, rows), a.dtype),
                pltpu.VMEM((SLOTS, tokens, WIDE), a.dtype),
                pltpu.VMEM((matrices * (pairs + 1), rows, WIDE), jnp.float32),
                pltpu.VMEM((2, units, half, TILE), a.dtype),
                pltpu.VMEM((GROUP - 1, 2, units, half, TILE), a.dtype),
                pltpu.SemaphoreType.DMA((2,)),
                pltpu.SemaphoreType.DMA((OPENING,)),
                pltpu.SemaphoreType.DMA((SLOTS,)),
                pltpu.SemaphoreType.DMA((OPENING,)),
                pltpu.SemaphoreType.DMA((2, HOPS, units)),
                pltpu.SemaphoreType.DMA((2, HOPS, units)),
            ],
            compiler_params=pltpu.CompilerParams(
                collective_id=0, has_side_effects=True, vmem_limit_bytes=57 * 2**20
            ),
            cost_estimate=pl.CostEstimate(
                flops=2 * matrices * tokens * rows * columns,
                bytes_accessed=2 * matrices * tokens * (rows + columns),
                transcendentals=0,
            ),
            name="sums",
        )(a, g)

    spec = jax.P(("rep", axis))
    return jax.shard_map(sums, mesh=mesh, in_specs=(spec, spec), out_specs=jax.P("rep"), check_vma=False)
```
